32 devices in a mesh: px: 4 (over y, x), py: 8 (over z, core).
Axes of the slice: x: 2, y: 2, z: 4, core: 2. Of those that a mesh axis runs over, the one named last changes fastest.
Arguments:
- velocity: float32 [3, 8, 256, 1024], P(None, None, 'py', 'px'), may hold values from -6 to 6
- thickness: float32 [8, 256, 1024], P(None, 'py', 'px'), may hold values from 1 to 4
- velocity_tendency: float32 [3, 8, 256, 1024], P(None, None, 'py', 'px'), may hold values from -6 to 6
- thickness_tendency: float32 [8, 256, 1024], P(None, 'py', 'px'), may hold values from -0.5 to 0.5
- cell_distance: float32 [3, 256, 1024], P(None, 'py', 'px'), may hold values from 0.5 to 2
- edge_length: float32 [3, 256, 1024], P(None, 'py', 'px'), may hold values from 0.5 to 2
- cell_area: float32 [256, 1024], P('py', 'px'), may hold values from 1 to 4
- kite_area: float32 [2, 3, 256, 1024], P(None, None, 'py', 'px'), may hold values from 0.2 to 0.8
- coriolis: float32 [2, 256, 1024], P(None, 'py', 'px'), may hold values from -1 to 1
Outputs:
- vertex_potential: float32 [2, 8, 256, 1024], P(None, None, 'py', 'px')
- kinetic_energy: float32 [8, 256, 1024], P(None, 'py', 'px')
- cell_potential: float32 [8, 256, 1024], P(None, 'py', 'px')
- edge_potential: float32 [3, 8, 256, 1024], P(None, None, 'py', 'px')
The draws below stay inside these ranges and needn't reach their ends.
All inputs are finite; a program needn't handle non-finite values.
Results may differ from the reference program's by a relative error of at most 0.00002.
Values sent between devices are 32-bit elements; how exact they have to be, the bound alone decides.
A program may use at most 64 MiB of HBM per device.

```python
import math
import jax
import jax.numpy as jnp

NLEV = 8
SECTIONS = 4
NX = 256
NY = 1024


def levels(key, shape, split, least, top_value):
    def one(position, blocks):
        draws = jax.random.uniform(jax.random.fold_in(jax.random.fold_in(key, 6), position), (blocks,), jnp.float32, least / len(split), top_value / len(split))
        return jnp.repeat(jnp.exp(draws), shape[position] // blocks).reshape((-1,) + (1,) * (len(shape) - position - 1))

    loudness = one(*split[0])
    for cut in split[1:]:
        loudness = loudness * one(*cut)
    return loudness


def noise(own_key, extent, scale, bound, shards=(), dtype=jnp.bfloat16):
    values = scale * jax.random.normal(own_key, extent, jnp.float32)
    if shards:
        values = values * levels(own_key, extent, shards, -0.22, 0.18)
    return jnp.clip(values, -bound, bound).astype(dtype)


def setup_inputs(seed: int = 0) -> dict:
    arg_keys = jax.random.split(jax.random.key(seed), 10)
    velocity = noise(arg_keys[0], (3, NLEV, NX, NY), 1.0, 6.0, ((2, 8), (3, 4)), jnp.float32)
    thickness = jnp.clip(jnp.exp(math.log(4.0) - 1.3862944 * jax.random.uniform(arg_keys[1], (NLEV, NX, NY), jnp.float32) ** levels(arg_keys[1], (NLEV, NX, NY), ((1, 8), (2, 4)), -0.2, 0.2)), 1.0, 4.0)
    velocity_tendency = noise(arg_keys[2], (3, NLEV, NX, NY), 1.0, 6.0, ((2, 8), (3, 4)), jnp.float32)
    thickness_tendency = jnp.clip(jax.random.uniform(arg_keys[3], (NLEV, NX, NY), jnp.float32, -0.5, 0.5) * levels(arg_keys[3], (NLEV, NX, NY), ((1, 8), (2, 4)), -0.4, 0.0), -0.5, 0.5)
    cell_distance = jnp.clip(jnp.exp(math.log(2.0) - 1.3862944 * jax.random.uniform(arg_keys[4], (3, NX, NY), jnp.float32) ** levels(arg_keys[4], (3, NX, NY), ((1, 8), (2, 4)), -0.2, 0.2)), 0.5, 2.0)
    edge_length = jnp.clip(jnp.exp(math.log(2.0) - 1.3862944 * jax.random.uniform(arg_keys[5], (3, NX, NY), jnp.float32) ** levels(arg_keys[5], (3, NX, NY), ((1, 8), (2, 4)), -0.2, 0.2)), 0.5, 2.0)
    cell_area = jnp.clip(jnp.exp(math.log(4.0) - 1.3862944 * jax.random.uniform(arg_keys[6], (NX, NY), jnp.float32) ** levels(arg_keys[6], (NX, NY), ((0, 8), (1, 4)), -0.2, 0.2)), 1.0, 4.0)
    kite_area = jnp.clip(jnp.exp(math.log(0.8) - 1.3862944 * jax.random.uniform(arg_keys[7], (2, 3, NX, NY), jnp.float32) ** levels(arg_keys[7], (2, 3, NX, NY), ((2, 8), (3, 4)), -0.2, 0.2)), 0.2, 0.8)
    coriolis = jnp.clip(jax.random.uniform(arg_keys[8], (2, NX, NY), jnp.float32, -1.0, 1.0) * levels(arg_keys[8], (2, NX, NY), ((1, 8), (2, 4)), -0.4, 0.0), -1.0, 1.0)
    return dict(velocity=velocity, thickness=thickness, velocity_tendency=velocity_tendency, thickness_tendency=thickness_tendency, cell_distance=cell_distance, edge_length=edge_length, cell_area=cell_area, kite_area=kite_area, coriolis=coriolis)


SECTION_STEP = (0.0, 0.5, 0.5, 1.0)
SECTION_WEIGHT = (1.0 / 6.0, 1.0 / 3.0, 1.0 / 3.0, 1.0 / 6.0)
UPWIND_FACTOR = 0.5


def neighbour(field, first_off, second_off):
    return jnp.roll(field, (-first_off, -second_off), axis=(-2, -1))


def reference(velocity, thickness, velocity_tendency, thickness_tendency, cell_distance, edge_length, cell_area, kite_area, coriolis):
    triangle_area = jnp.sum(kite_area, axis=1)
    edge_weight = 0.25 * cell_distance * edge_length
    vertex_total = jnp.zeros((2,) + thickness.shape, jnp.float32)
    energy_total = jnp.zeros(thickness.shape, jnp.float32)
    cell_total = jnp.zeros(thickness.shape, jnp.float32)
    edge_total = jnp.zeros(velocity.shape, jnp.float32)
    for section_index in range(SECTIONS):
        step_size = SECTION_STEP[section_index]
        weight_now = SECTION_WEIGHT[section_index]
        section_velocity = velocity + step_size * velocity_tendency
        section_thickness = thickness + step_size * thickness_tendency
        edge_flux = section_velocity * cell_distance[:, None]
        circulation_first = edge_flux[0] + neighbour(edge_flux[2], 1, 0) - edge_flux[1]
        circulation_second = edge_flux[1] - edge_flux[2] - neighbour(edge_flux[0], -1, 1)
        height_first = (kite_area[0, 0] * section_thickness + kite_area[0, 1] * neighbour(section_thickness, 1, 0)
                        + kite_area[0, 2] * neighbour(section_thickness, 0, 1)) / triangle_area[0]
        height_second = (kite_area[1, 0] * section_thickness + kite_area[1, 1] * neighbour(section_thickness, 0, 1)
                         + kite_area[1, 2] * neighbour(section_thickness, -1, 1)) / triangle_area[1]
        potential_first = (coriolis[0] + circulation_first / triangle_area[0]) / height_first
        potential_second = (coriolis[1] + circulation_second / triangle_area[1]) / height_second
        energy = edge_weight[:, None] * section_velocity * section_velocity
        kinetic = (energy[0] + energy[1] + energy[2] + neighbour(energy[0], -1, 0)
                   + neighbour(energy[1], 0, -1) + neighbour(energy[2], 1, -1)) / cell_area
        cell_value = (potential_first + potential_second + neighbour(potential_first, -1, 0)
                      + neighbour(potential_first, 0, -1) + neighbour(potential_second, 0, -1)
                      + neighbour(potential_second, 1, -1)) / 6.0
        mean_zero = 0.5 * (potential_first + neighbour(potential_second, 1, -1))
        mean_one = 0.5 * (potential_first + potential_second)
        mean_two = 0.5 * (potential_second + neighbour(potential_first, -1, 0))
        grad_zero = (neighbour(cell_value, 1, 0) - cell_value) / cell_distance[0]
        grad_one = (neighbour(cell_value, 0, 1) - cell_value) / cell_distance[1]
        grad_two = (neighbour(cell_value, -1, 1) - cell_value) / cell_distance[2]
        section_edge = jnp.stack([
            mean_zero - UPWIND_FACTOR * section_velocity[0] * grad_zero,
            mean_one - UPWIND_FACTOR * section_velocity[1] * grad_one,
            mean_two - UPWIND_FACTOR * section_velocity[2] * grad_two])
        vertex_total = vertex_total + weight_now * jnp.stack([potential_first, potential_second])
        energy_total = energy_total + weight_now * kinetic
        cell_total = cell_total + weight_now * cell_value
        edge_total = edge_total + weight_now * section_edge
    return vertex_total, energy_total, cell_total, edge_total
```

```python
import jax
import jax.numpy as jnp
from jax import lax
from jax.experimental import pallas as pl
from jax.experimental.pallas import tpu as pltpu
from jax.sharding import PartitionSpec as P

SUB = 8
LANE = 128
COMPS = 8
GEO = 14
LANE_STEP = 2 * COMPS
MESH = pl.DeviceIdType.MESH


def iotas():
    sub = lax.broadcasted_iota(jnp.int32, (SUB, LANE), 0)
    lane = lax.broadcasted_iota(jnp.int32, (SUB, LANE), 1)
    return sub, lane


def exchange_kernel(counts, *refs):
    (vel, th, vt, tt, cd, el, kite, cor) = refs[:8]
    (o_bot, o_top, o_right, o_left, o_br, o_tr, o_bl) = refs[8:15]
    bufs = refs[15:23]
    (p_bot, p_top, p_right, p_left) = refs[23:27]
    in_sem, send_sem, recv_sem = refs[27:30]
    ny, nx = counts
    py, px = lax.axis_index("py"), lax.axis_index("px")
    down, up = lax.rem(py + 1, ny), lax.rem(py + ny - 1, ny)
    right, left = lax.rem(px + 1, nx), lax.rem(px + nx - 1, nx)

    loads = [
        pltpu.make_async_copy(src, dst, in_sem.at[i])
        for i, (src, dst) in enumerate(zip((vel, th, vt, tt, cd, el, kite, cor), bufs))
    ]
    for i in (4, 5, 6, 7, 0, 1, 2, 3):
        loads[i].start()
    barrier = pltpu.get_barrier_semaphore()
    near = [
        (up, px), (down, px), (py, left), (py, right),
        (up, left), (up, right), (down, left), (down, right),
    ]
    for y, x in near:
        pl.semaphore_signal(barrier, inc=1, device_id={"py": y, "px": x}, device_id_type=MESH)

    b_vel, b_th, b_vt, b_tt, b_cd, b_el, b_kite, b_cor = bufs
    levels, rows, cols = b_th.shape
    nr, nc = rows // SUB, cols // LANE
    sub, lane = iotas()
    last = slice(cols - LANE, cols)

    def view(ref, *lead):
        return lambda r, c: ref[lead + (r, c)]

    def level_comps(l):
        return (
            [view(b_vel, k, l) for k in range(3)]
            + [view(b_th, l)]
            + [view(b_vt, k, l) for k in range(3)]
            + [view(b_tt, l)]
        )

    geo = (
        [view(b_cd, k) for k in range(3)]
        + [view(b_el, k) for k in range(3)]
        + [view(b_kite, v, k) for v in range(2) for k in range(3)]
        + [view(b_cor, v) for v in range(2)]
    )

    def pack_rows(comps, base):
        for g in range(0, len(comps), 4):
            for c in range(nc):
                cs = slice(c * LANE, (c + 1) * LANE)
                bot = top = jnp.zeros((SUB, LANE), jnp.float32)
                for q, f in enumerate(comps[g : g + 4]):
                    m = jnp.where(sub < 4, f(slice(0, SUB), cs), f(slice(rows - SUB, rows), cs))
                    m = pltpu.roll(m, 2 * q, 0) if q else m
                    bot = jnp.where((sub == 2 * q) | (sub == 2 * q + 1), m, bot)
                    t = (2 * q + 6) % SUB
                    top = jnp.where((sub == t) | (sub == t + 1), m, top)
                at = slice(base + 2 * g, base + 2 * g + SUB)
                p_bot[at, cs] = bot
                p_top[at, cs] = top

    def pack_cols(items, tile):
        for r in range(nr):
            rs = slice(r * SUB, (r + 1) * SUB)
            ra = la = jnp.zeros((SUB, LANE), jnp.float32)
            for s, f in items:
                m = jnp.where(lane < LANE // 2, f(rs, slice(0, LANE)), f(rs, last))
                m = pltpu.roll(m, s, 1) if s else m
                ra = jnp.where((lane == s) | (lane == s + 1), m, ra)
                la = jnp.where(lane == (s + LANE - 1) % LANE, m, la)
            cs = slice(tile * LANE, (tile + 1) * LANE)
            p_right[rs, cs] = ra
            p_left[rs, cs] = la

    for i in (4, 5, 6, 7):
        loads[i].wait()
    pack_rows(geo, levels * LANE_STEP)
    pack_cols([(2 * k, f) for k, f in enumerate(geo)], 1)
    for i in (0, 1, 2, 3):
        loads[i].wait()
    items = []
    for l in range(levels):
        comps = level_comps(l)
        items += [(l * LANE_STEP + 2 * k, f) for k, f in enumerate(comps)]
    pack_cols(items, 0)
    for l in range(levels):
        pack_rows(level_comps(l), l * LANE_STEP)

    pl.semaphore_wait(barrier, len(near))
    plan = [
        (p_bot, o_bot, (up, px)),
        (p_top, o_top, (down, px)),
        (p_right.at[rows - SUB : rows], o_tr, (down, left)),
        (p_right.at[0:SUB], o_br, (up, left)),
        (p_left.at[0:SUB], o_bl, (up, right)),
        (p_right, o_right, (py, left)),
        (p_left, o_left, (py, right)),
    ]
    copies = [
        pltpu.make_async_remote_copy(
            src_ref=src,
            dst_ref=dst,
            send_sem=send_sem.at[i],
            recv_sem=recv_sem.at[i],
            device_id={"py": y, "px": x},
            device_id_type=MESH,
        )
        for i, (src, dst, (y, x)) in enumerate(plan)
    ]
    for copy in copies:
        copy.start()
    for copy in copies:
        copy.wait()


def exchange(counts, vel, th, vt, tt, cd, el, kite, cor):
    levels, rows, cols = th.shape
    f32 = jnp.float32
    band = (levels * LANE_STEP + 32, cols)
    side = (rows, 2 * LANE)
    corner = (SUB, 2 * LANE)
    args = (vel, th, vt, tt, cd, el, kite, cor)
    outs = (band, band, side, side, corner, corner, corner)
    return pl.pallas_call(
        lambda *refs: exchange_kernel(counts, *refs),
        out_shape=[jax.ShapeDtypeStruct(s, f32) for s in outs],
        in_specs=[pl.BlockSpec(memory_space=pl.ANY)] * len(args),
        out_specs=[pl.BlockSpec(memory_space=pl.ANY)] * len(outs),
        scratch_shapes=[pltpu.VMEM(a.shape, f32) for a in args]
        + [pltpu.VMEM(s, f32) for s in (band, band, side, side)]
        + [
            pltpu.SemaphoreType.DMA((len(args),)),
            pltpu.SemaphoreType.DMA((len(outs),)),
            pltpu.SemaphoreType.DMA((len(outs),)),
        ],
        compiler_params=pltpu.CompilerParams(collective_id=0, has_side_effects=True),
        name="exchange",
    )(*args)


class Field:
    def __init__(self, grid, make):
        self.grid, self.make, self.memo = grid, make, {}

    def __call__(self, r, c):
        key = (r % self.grid[0], c % self.grid[1])
        if key not in self.memo:
            self.memo[key] = self.make(*key)
        return self.memo[key]


def step_kernel(
    vel, th, vt, tt, cd, el, kite, cor, area,
    bot, top, gbot, gtop, right, left, br, tr, bl,
    o_vert, o_kin, o_cell, o_edge, geo, scale,
):
    level = pl.program_id(0)
    rows, cols = area.shape
    nr, nc = rows // SUB, cols // LANE
    grid = (nr + 1, nc + 1)
    sub, lane = iotas()

    def at(r, c):
        return (slice(r * SUB, (r + 1) * SUB), slice(c * LANE, (c + 1) * LANE))

    def lift(fn, *fields):
        return Field(grid, lambda r, c: fn(*[f(r, c) for f in fields]))

    def row_shift(f, a):
        rolled = Field(grid, lambda r, c: pltpu.roll(f(r, c), (-a) % SUB, 0))
        if a == 1:
            return Field(grid, lambda r, c: jnp.where(sub < SUB - 1, rolled(r, c), rolled(r + 1, c)))
        return Field(grid, lambda r, c: jnp.where(sub > 0, rolled(r, c), rolled(r - 1, c)))

    def col_shift(f, b):
        rolled = Field(grid, lambda r, c: pltpu.roll(f(r, c), (-b) % LANE, 1))
        if b == 1:
            return Field(grid, lambda r, c: jnp.where(lane < LANE - 1, rolled(r, c), rolled(r, c + 1)))
        return Field(grid, lambda r, c: jnp.where(lane > 0, rolled(r, c), rolled(r, c - 1)))

    def extended(own, k, band_bot, band_top, side):
        q, g = k % 4, k // 4

        def make(r, c):
            if r < nr and c < nc:
                return own(*at(r, c))
            if c < nc:
                b, t = band_bot[at(g, c)], band_top[at(g, c)]
                m = jnp.where((sub == 2 * q) | (sub == 2 * q + 1), b, t)
                return pltpu.roll(m, (-2 * q) % SUB, 0) if q else m
            rt, lt = side(r)
            m = jnp.where((lane == 2 * k) | (lane == 2 * k + 1), rt, lt)
            return pltpu.roll(m, (-2 * k) % LANE, 1) if k else m

        return Field(grid, make)

    def side_of(tile, turn):
        cs = slice(tile * LANE, (tile + 1) * LANE)
        memo = {}

        def side(r):
            if r not in memo:
                if r < nr:
                    rs = slice(r * SUB, (r + 1) * SUB)
                    pair = right[rs, cs], left[rs, cs]
                else:
                    pair = jnp.where(sub < 4, br[:, cs], tr[:, cs]), bl[:, cs]
                memo[r] = tuple(turn(x) for x in pair)
            return memo[r]

        return side

    def view(ref, *lead):
        return lambda r, c: ref[lead + (r, c)]

    @pl.when(level == 0)
    def _():
        side = side_of(1, lambda x: x)
        owns = (
            [view(cd, k) for k in range(3)]
            + [view(el, k) for k in range(3)]
            + [view(kite, v, k) for v in range(2) for k in range(3)]
            + [view(cor, v) for v in range(2)]
        )
        f = [extended(own, k, gbot, gtop, side) for k, own in enumerate(owns)]
        for r in range(nr + 1):
            for c in range(nc + 1):
                for k in range(3):
                    geo[(k,) + at(r, c)] = f[k](r, c)
                    geo[(3 + k,) + at(r, c)] = 0.25 * f[k](r, c) * f[3 + k](r, c)
                for k in range(6):
                    geo[(6 + k,) + at(r, c)] = f[6 + k](r, c)
                for v in range(2):
                    t = f[6 + 3 * v](r, c) + f[7 + 3 * v](r, c) + f[8 + 3 * v](r, c)
                    geo[(12 + v,) + at(r, c)] = f[12 + v](r, c) * t
                if r < nr and c < nc:
                    for k in range(3):
                        scale[(k,) + at(r, c)] = (-0.5 / 36.0) / f[k](r, c)
                    scale[(3,) + at(r, c)] = 1.0 / area[at(r, c)]

    turn_by = lax.rem(LANE - level * LANE_STEP, LANE)
    side = side_of(0, lambda x: pltpu.roll(x, turn_by, 1))
    owns = (
        [view(vel, k, 0) for k in range(3)]
        + [view(th, 0)]
        + [view(vt, k, 0) for k in range(3)]
        + [view(tt, 0)]
    )
    x = [extended(own, k, bot, top, side) for k, own in enumerate(owns)]
    v, h, t, g = x[0:3], x[3], x[4:7], x[7]

    def geo_tile(k):
        return lambda r, c: geo[(k,) + at(r % grid[0], c % grid[1])]

    dist = [geo_tile(k) for k in range(3)]
    ew = [geo_tile(3 + k) for k in range(3)]
    kt = [geo_tile(6 + k) for k in range(6)]
    ct = [geo_tile(12 + k) for k in range(2)]

    def parts(vv, hh):
        flux = [lift(lambda a, b: a * b, vv[k], dist[k]) for k in range(3)]
        c0 = lift(lambda a, b, c: a + b - c, flux[0], row_shift(flux[2], 1), flux[1])
        c1 = lift(
            lambda a, b, c: a - b - c, flux[1], flux[2], col_shift(row_shift(flux[0], -1), 1)
        )
        hc = col_shift(hh, 1)
        hr = row_shift(hh, 1)
        hd = row_shift(hc, -1)
        mix = lambda a, b, c, p, q, s: a * p + b * q + c * s
        h0 = lift(mix, kt[0], kt[1], kt[2], hh, hr, hc)
        h1 = lift(mix, kt[3], kt[4], kt[5], hh, hc, hd)
        return (c0, c1), (h0, h1)

    cv, hv = parts(v, h)
    cw, hw = parts(t, g)

    def potential(k):
        def make(r, c):
            a0 = ct[k](r, c) + cv[k](r, c)
            a1 = cw[k](r, c)
            b0 = hv[k](r, c)
            b1 = hw[k](r, c)
            first = a0 / b0
            mid = (a0 + 0.5 * a1) / (b0 + 0.5 * b1)
            end = (a0 + a1) / (b0 + b1)
            late = 2.0 * mid + end
            return first + 2.0 * mid + late, late

        both = Field(grid, make)
        return Field(grid, lambda r, c: both(r, c)[0]), Field(grid, lambda r, c: both(r, c)[1])

    p0, q0 = potential(0)
    p1, q1 = potential(1)
    add = lambda a, b: a + b
    add3 = lambda a, b, c: a + b + c

    def cell(f0, f1):
        f0_up = row_shift(f0, -1)
        f1_down = row_shift(f1, 1)
        pair = lift(add, f0, f1)
        return lift(add3, pair, f0_up, col_shift(lift(add, pair, f1_down), -1)), f0_up, f1_down, pair

    cc, p0_up, p1_down, pair = cell(p0, p1)
    dd = cell(q0, q1)[0]
    p1_low = col_shift(p1_down, -1)

    def neighbours(f):
        fc = col_shift(f, 1)
        return row_shift(f, 1), fc, row_shift(fc, -1)

    cn, dn = neighbours(cc), neighbours(dd)
    ends = [lift(add, p0, p1_low), pair, lift(add, p1, p0_up)]
    en = [
        lift(lambda w, a, b: w * (a * (a + b) + (1.0 / 3.0) * (b * b)), ew[k], v[k], t[k])
        for k in range(3)
    ]
    e_up = row_shift(en[0], -1)
    e_low = col_shift(lift(add, en[1], row_shift(en[2], 1)), -1)

    for r in range(nr):
        for c in range(nc):
            p = at(r, c)
            o_vert[(0, 0) + p] = p0(r, c) * (1.0 / 6.0)
            o_vert[(1, 0) + p] = p1(r, c) * (1.0 / 6.0)
            total = en[0](r, c) + en[1](r, c) + en[2](r, c) + e_up(r, c) + e_low(r, c)
            o_kin[(0,) + p] = total * scale[(3,) + p]
            o_cell[(0,) + p] = cc(r, c) * (1.0 / 36.0)
            for k in range(3):
                slope = v[k](r, c) * (cn[k](r, c) - cc(r, c)) + t[k](r, c) * (dn[k](r, c) - dd(r, c))
                o_edge[(k, 0) + p] = ends[k](r, c) * (1.0 / 12.0) + scale[(k,) + p] * slope


def local(counts, vel, th, vt, tt, cd, el, area, kite, cor):
    bot, top, right, left, br, tr, bl = exchange(counts, vel, th, vt, tt, cd, el, kite, cor)
    levels, rows, cols = th.shape
    f32 = jnp.float32
    whole = lambda a: pl.BlockSpec(a.shape, lambda l: (0,) * a.ndim)
    three = pl.BlockSpec((3, 1, rows, cols), lambda l: (0, l, 0, 0))
    two = pl.BlockSpec((2, 1, rows, cols), lambda l: (0, l, 0, 0))
    one = pl.BlockSpec((1, rows, cols), lambda l: (l, 0, 0))
    band = pl.BlockSpec((LANE_STEP, cols), lambda l: (l, 0))
    gband = pl.BlockSpec((32, cols), lambda l: (levels * LANE_STEP // 32, 0))
    return pl.pallas_call(
        step_kernel,
        grid=(levels,),
        out_shape=[
            jax.ShapeDtypeStruct((2, levels, rows, cols), f32),
            jax.ShapeDtypeStruct((levels, rows, cols), f32),
            jax.ShapeDtypeStruct((levels, rows, cols), f32),
            jax.ShapeDtypeStruct((3, levels, rows, cols), f32),
        ],
        in_specs=[
            three, one, three, one, whole(cd), whole(el), whole(kite), whole(cor), whole(area),
            band, band, gband, gband, whole(right), whole(left), whole(br), whole(tr), whole(bl),
        ],
        out_specs=[two, one, one, three],
        scratch_shapes=[
            pltpu.VMEM((GEO, rows + SUB, cols + LANE), f32),
            pltpu.VMEM((4, rows, cols), f32),
        ],
        name="step",
    )(vel, th, vt, tt, cd, el, kite, cor, area, bot, top, bot, top, right, left, br, tr, bl)


def solution(mesh):
    counts = (mesh.shape["py"], mesh.shape["px"])
    p4, p3 = P(None, None, "py", "px"), P(None, "py", "px")
    return jax.shard_map(
        lambda *args: local(counts, *args),
        mesh=mesh,
        in_specs=(p4, p3, p4, p3, p3, p3, P("py", "px"), p4, p3),
        out_specs=(p4, p3, p3, p4),
        check_vma=False,
    )
```

```python
import jax
import jax.numpy as jnp
from jax import lax
from jax.experimental import pallas as pl
from jax.experimental.pallas import tpu as pltpu
from jax.sharding import PartitionSpec as P

SUB = 8
LANE = 128
COMPS = 8
GEO = 14
DEPTH = 2
LANE_STEP = 2 * COMPS
MESH = pl.DeviceIdType.MESH


def iotas():
    sub = lax.broadcasted_iota(jnp.int32, (SUB, LANE), 0)
    lane = lax.broadcasted_iota(jnp.int32, (SUB, LANE), 1)
    return sub, lane


def exchange_kernel(counts, *refs):
    (vel, th, vt, tt, cd, el, kite, cor) = refs[:8]
    (o_bot, o_top, o_right, o_left, o_br, o_tr, o_bl) = refs[8:15]
    bufs = refs[15:23]
    (p_bot, p_top, p_right, p_left) = refs[23:27]
    in_sem, send_sem, recv_sem = refs[27:30]
    ny, nx = counts
    py, px = lax.axis_index("py"), lax.axis_index("px")
    down, up = lax.rem(py + 1, ny), lax.rem(py + ny - 1, ny)
    right, left = lax.rem(px + 1, nx), lax.rem(px + nx - 1, nx)

    loads = [
        pltpu.make_async_copy(src, dst, in_sem.at[i])
        for i, (src, dst) in enumerate(zip((vel, th, vt, tt, cd, el, kite, cor), bufs))
    ]
    for i in (4, 5, 6, 7, 0, 1, 2, 3):
        loads[i].start()
    barrier = pltpu.get_barrier_semaphore()
    near = [
        (up, px), (down, px), (py, left), (py, right),
        (up, left), (up, right), (down, left), (down, right),
    ]
    for y, x in near:
        pl.semaphore_signal(barrier, inc=1, device_id={"py": y, "px": x}, device_id_type=MESH)

    b_vel, b_th, b_vt, b_tt, b_cd, b_el, b_kite, b_cor = bufs
    levels, rows, cols = b_th.shape
    nr, nc = rows // SUB, cols // LANE
    sub, lane = iotas()
    last = slice(cols - LANE, cols)

    def view(ref, *lead):
        return lambda r, c: ref[lead + (r, c)]

    def level_comps(l):
        return (
            [view(b_vel, k, l) for k in range(3)]
            + [view(b_th, l)]
            + [view(b_vt, k, l) for k in range(3)]
            + [view(b_tt, l)]
        )

    geo = (
        [view(b_cd, k) for k in range(3)]
        + [view(b_el, k) for k in range(3)]
        + [view(b_kite, v, k) for v in range(2) for k in range(3)]
        + [view(b_cor, v) for v in range(2)]
    )

    def pack_rows(comps, base):
        for g in range(0, len(comps), 4):
            for c in range(nc):
                cs = slice(c * LANE, (c + 1) * LANE)
                bot = top = jnp.zeros((SUB, LANE), jnp.float32)
                for q, f in enumerate(comps[g : g + 4]):
                    m = jnp.where(sub < 4, f(slice(0, SUB), cs), f(slice(rows - SUB, rows), cs))
                    m = pltpu.roll(m, 2 * q, 0) if q else m
                    bot = jnp.where((sub == 2 * q) | (sub == 2 * q + 1), m, bot)
                    t = (2 * q + 6) % SUB
                    top = jnp.where((sub == t) | (sub == t + 1), m, top)
                at = slice(base + 2 * g, base + 2 * g + SUB)
                p_bot[at, cs] = bot
                p_top[at, cs] = top

    def pack_cols(items, tile):
        for r in range(nr):
            rs = slice(r * SUB, (r + 1) * SUB)
            ra = la = jnp.zeros((SUB, LANE), jnp.float32)
            for s, f in items:
                m = jnp.where(lane < LANE // 2, f(rs, slice(0, LANE)), f(rs, last))
                m = pltpu.roll(m, s, 1) if s else m
                ra = jnp.where((lane == s) | (lane == s + 1), m, ra)
                la = jnp.where(lane == (s + LANE - 1) % LANE, m, la)
            cs = slice(tile * LANE, (tile + 1) * LANE)
            p_right[rs, cs] = ra
            p_left[rs, cs] = la

    plan = [
        (p_bot, o_bot, (up, px)),
        (p_top, o_top, (down, px)),
        (p_right.at[rows - SUB : rows], o_tr, (down, left)),
        (p_right.at[0:SUB], o_br, (up, left)),
        (p_left.at[0:SUB], o_bl, (up, right)),
        (p_right, o_right, (py, left)),
        (p_left, o_left, (py, right)),
    ]
    copies = [
        pltpu.make_async_remote_copy(
            src_ref=src,
            dst_ref=dst,
            send_sem=send_sem.at[i],
            recv_sem=recv_sem.at[i],
            device_id={"py": y, "px": x},
            device_id_type=MESH,
        )
        for i, (src, dst, (y, x)) in enumerate(plan)
    ]
    for i in (4, 5, 6, 7):
        loads[i].wait()
    pack_rows(geo, levels * LANE_STEP)
    pack_cols([(2 * k, f) for k, f in enumerate(geo)], 1)
    for i in (0, 1, 2, 3):
        loads[i].wait()
    for l in range(levels):
        pack_rows(level_comps(l), l * LANE_STEP)
    pl.semaphore_wait(barrier, len(near))
    for copy in copies[:2]:
        copy.start()
    items = []
    for l in range(levels):
        comps = level_comps(l)
        items += [(l * LANE_STEP + 2 * k, f) for k, f in enumerate(comps)]
    pack_cols(items, 0)
    for copy in copies[2:]:
        copy.start()
    for copy in copies:
        copy.wait()


def exchange(counts, vel, th, vt, tt, cd, el, kite, cor):
    levels, rows, cols = th.shape
    f32 = jnp.float32
    band = (levels * LANE_STEP + 32, cols)
    side = (rows, 2 * LANE)
    corner = (SUB, 2 * LANE)
    args = (vel, th, vt, tt, cd, el, kite, cor)
    outs = (band, band, side, side, corner, corner, corner)
    return pl.pallas_call(
        lambda *refs: exchange_kernel(counts, *refs),
        out_shape=[jax.ShapeDtypeStruct(s, f32) for s in outs],
        in_specs=[pl.BlockSpec(memory_space=pl.ANY)] * len(args),
        out_specs=[pl.BlockSpec(memory_space=pl.ANY)] * len(outs),
        scratch_shapes=[pltpu.VMEM(a.shape, f32) for a in args]
        + [pltpu.VMEM(s, f32) for s in (band, band, side, side)]
        + [
            pltpu.SemaphoreType.DMA((len(args),)),
            pltpu.SemaphoreType.DMA((len(outs),)),
            pltpu.SemaphoreType.DMA((len(outs),)),
        ],
        compiler_params=pltpu.CompilerParams(collective_id=0, has_side_effects=True),
        name="exchange",
    )(*args)


class Field:
    def __init__(self, grid, make):
        self.grid, self.make, self.memo = grid, make, {}

    def __call__(self, r, c):
        key = (r % self.grid[0], c % self.grid[1])
        if key not in self.memo:
            self.memo[key] = self.make(*key)
        return self.memo[key]


def step_kernel(
    vel, th, vt, tt, cd, el, kite, cor, area,
    bot, top, gbot, gtop, right, left, br, tr, bl,
    o_vert, o_kin, o_cell, o_edge, geo, scale,
):
    level = pl.program_id(0)
    rows, cols = area.shape
    nr, nc = rows // SUB, cols // LANE
    grid = (nr + 1, nc + 1)
    sub, lane = iotas()

    def at(r, c):
        return (slice(r * SUB, (r + 1) * SUB), slice(c * LANE, (c + 1) * LANE))

    def lift(fn, *fields):
        return Field(grid, lambda r, c: fn(*[f(r, c) for f in fields]))

    def row_shift(f, a):
        rolled = Field(grid, lambda r, c: pltpu.roll(f(r, c), (-a) % SUB, 0))
        if a == 1:
            return Field(grid, lambda r, c: jnp.where(sub < SUB - 1, rolled(r, c), rolled(r + 1, c)))
        return Field(grid, lambda r, c: jnp.where(sub > 0, rolled(r, c), rolled(r - 1, c)))

    def col_shift(f, b):
        rolled = Field(grid, lambda r, c: pltpu.roll(f(r, c), (-b) % LANE, 1))
        if b == 1:
            return Field(grid, lambda r, c: jnp.where(lane < LANE - 1, rolled(r, c), rolled(r, c + 1)))
        return Field(grid, lambda r, c: jnp.where(lane > 0, rolled(r, c), rolled(r, c - 1)))

    def extended(own, k, band_bot, band_top, side):
        q, g = k % 4, k // 4

        def make(r, c):
            if c < nc:
                b, t = band_bot[at(g, c)], band_top[at(g, c)]
                m = jnp.where((sub == 2 * q) | (sub == 2 * q + 1), b, t)
                return pltpu.roll(m, (-2 * q) % SUB, 0) if q else m
            rt, lt = side(r)
            m = jnp.where((lane == 2 * k) | (lane == 2 * k + 1), rt, lt)
            return pltpu.roll(m, (-2 * k) % LANE, 1) if k else m

        halo = Field(grid, make)

        def tile(r, c):
            r, c = r % grid[0], c % grid[1]
            return own(*at(r, c)) if r < nr and c < nc else halo(r, c)

        return tile

    def side_of(tile, turn):
        cs = slice(tile * LANE, (tile + 1) * LANE)
        memo = {}

        def side(r):
            if r not in memo:
                if r < nr:
                    rs = slice(r * SUB, (r + 1) * SUB)
                    pair = right[rs, cs], left[rs, cs]
                else:
                    pair = jnp.where(sub < 4, br[:, cs], tr[:, cs]), bl[:, cs]
                memo[r] = tuple(turn(x) for x in pair)
            return memo[r]

        return side

    def view(ref, *lead):
        return lambda r, c: ref[lead + (r, c)]

    @pl.when(level == 0)
    def _():
        side = side_of(1, lambda x: x)
        owns = (
            [view(cd, k) for k in range(3)]
            + [view(el, k) for k in range(3)]
            + [view(kite, v, k) for v in range(2) for k in range(3)]
            + [view(cor, v) for v in range(2)]
        )
        f = [extended(own, k, gbot, gtop, side) for k, own in enumerate(owns)]
        for r in range(nr + 1):
            for c in range(nc + 1):
                for k in range(3):
                    geo[(k,) + at(r, c)] = f[k](r, c)
                    geo[(3 + k,) + at(r, c)] = 0.25 * f[k](r, c) * f[3 + k](r, c)
                for k in range(6):
                    geo[(6 + k,) + at(r, c)] = f[6 + k](r, c)
                for v in range(2):
                    t = f[6 + 3 * v](r, c) + f[7 + 3 * v](r, c) + f[8 + 3 * v](r, c)
                    geo[(12 + v,) + at(r, c)] = f[12 + v](r, c) * t
                if r < nr and c < nc:
                    for k in range(3):
                        scale[(k,) + at(r, c)] = (-0.5 / 36.0) / f[k](r, c)
                    scale[(3,) + at(r, c)] = 1.0 / area[at(r, c)]

    turn_by = lax.rem(LANE - level * (DEPTH * LANE_STEP), LANE)
    side = side_of(0, lambda x: pltpu.roll(x, turn_by, 1))
    for u in range(DEPTH):
        owns = (
            [view(vel, k, u) for k in range(3)]
            + [view(th, u)]
            + [view(vt, k, u) for k in range(3)]
            + [view(tt, u)]
        )
        x = [extended(own, u * COMPS + k, bot, top, side) for k, own in enumerate(owns)]
        v, h, t, g = x[0:3], x[3], x[4:7], x[7]

        def geo_tile(k):
            return lambda r, c: geo[(k,) + at(r % grid[0], c % grid[1])]

        dist = [geo_tile(k) for k in range(3)]
        ew = [geo_tile(3 + k) for k in range(3)]
        kt = [geo_tile(6 + k) for k in range(6)]
        ct = [geo_tile(12 + k) for k in range(2)]

        def parts(vv, hh):
            flux = [lift(lambda a, b: a * b, vv[k], dist[k]) for k in range(3)]
            c0 = lift(lambda a, b, c: a + b - c, flux[0], row_shift(flux[2], 1), flux[1])
            c1 = lift(
                lambda a, b, c: a - b - c, flux[1], flux[2], col_shift(row_shift(flux[0], -1), 1)
            )
            hc = col_shift(hh, 1)
            hr = row_shift(hh, 1)
            hd = row_shift(hc, -1)
            mix = lambda a, b, c, p, q, s: a * p + b * q + c * s
            h0 = lift(mix, kt[0], kt[1], kt[2], hh, hr, hc)
            h1 = lift(mix, kt[3], kt[4], kt[5], hh, hc, hd)
            return (c0, c1), (h0, h1)

        cv, hv = parts(v, h)
        cw, hw = parts(t, g)

        def potential(k):
            def make(r, c):
                a0 = ct[k](r, c) + cv[k](r, c)
                a1 = cw[k](r, c)
                b0 = hv[k](r, c)
                b1 = hw[k](r, c)
                bm, be = b0 + 0.5 * b1, b0 + b1
                m = bm * be
                scale_all = 1.0 / (b0 * m)
                mid = (a0 + a0 + a1) * (b0 * be)
                late = mid + (a0 + a1) * (b0 * bm)
                return (a0 * m + mid + late) * scale_all, late * scale_all

            both = Field(grid, make)
            return Field(grid, lambda r, c: both(r, c)[0]), Field(grid, lambda r, c: both(r, c)[1])

        p0, q0 = potential(0)
        p1, q1 = potential(1)
        add = lambda a, b: a + b
        add3 = lambda a, b, c: a + b + c

        def cell(f0, f1):
            f0_up = row_shift(f0, -1)
            f1_down = row_shift(f1, 1)
            pair = lift(add, f0, f1)
            return lift(add3, pair, f0_up, col_shift(lift(add, pair, f1_down), -1)), f0_up, f1_down, pair

        cc, p0_up, p1_down, pair = cell(p0, p1)
        dd = cell(q0, q1)[0]
        p1_low = col_shift(p1_down, -1)

        def neighbours(f):
            fc = col_shift(f, 1)
            return row_shift(f, 1), fc, row_shift(fc, -1)

        cn, dn = neighbours(cc), neighbours(dd)
        ends = [lift(add, p0, p1_low), pair, lift(add, p1, p0_up)]
        en = [
            lift(lambda w, a, b: w * (a * (a + b) + (1.0 / 3.0) * (b * b)), ew[k], v[k], t[k])
            for k in range(3)
        ]
        e_up = row_shift(en[0], -1)
        e_low = col_shift(lift(add, en[1], row_shift(en[2], 1)), -1)

        for r in range(nr):
            for c in range(nc):
                p = at(r, c)
                o_vert[(0, u) + p] = p0(r, c) * (1.0 / 6.0)
                o_vert[(1, u) + p] = p1(r, c) * (1.0 / 6.0)
                total = en[0](r, c) + en[1](r, c) + en[2](r, c) + e_up(r, c) + e_low(r, c)
                o_kin[(u,) + p] = total * scale[(3,) + p]
                o_cell[(u,) + p] = cc(r, c) * (1.0 / 36.0)
                for k in range(3):
                    slope = v[k](r, c) * (cn[k](r, c) - cc(r, c)) + t[k](r, c) * (dn[k](r, c) - dd(r, c))
                    o_edge[(k, u) + p] = ends[k](r, c) * (1.0 / 12.0) + scale[(k,) + p] * slope


def local(counts, vel, th, vt, tt, cd, el, area, kite, cor):
    bot, top, right, left, br, tr, bl = exchange(counts, vel, th, vt, tt, cd, el, kite, cor)
    levels, rows, cols = th.shape
    f32 = jnp.float32
    whole = lambda a: pl.BlockSpec(a.shape, lambda l: (0,) * a.ndim)
    three = pl.BlockSpec((3, DEPTH, rows, cols), lambda l: (0, l, 0, 0))
    two = pl.BlockSpec((2, DEPTH, rows, cols), lambda l: (0, l, 0, 0))
    one = pl.BlockSpec((DEPTH, rows, cols), lambda l: (l, 0, 0))
    band = pl.BlockSpec((DEPTH * LANE_STEP, cols), lambda l: (l, 0))
    gband = pl.BlockSpec((32, cols), lambda l: (levels * LANE_STEP // 32, 0))
    return pl.pallas_call(
        step_kernel,
        grid=(levels // DEPTH,),
        out_shape=[
            jax.ShapeDtypeStruct((2, levels, rows, cols), f32),
            jax.ShapeDtypeStruct((levels, rows, cols), f32),
            jax.ShapeDtypeStruct((levels, rows, cols), f32),
            jax.ShapeDtypeStruct((3, levels, rows, cols), f32),
        ],
        in_specs=[
            three, one, three, one, whole(cd), whole(el), whole(kite), whole(cor), whole(area),
            band, band, gband, gband, whole(right), whole(left), whole(br), whole(tr), whole(bl),
        ],
        out_specs=[two, one, one, three],
        scratch_shapes=[
            pltpu.VMEM((GEO, rows + SUB, cols + LANE), f32),
            pltpu.VMEM((4, rows, cols), f32),
        ],
        name="step",
    )(vel, th, vt, tt, cd, el, kite, cor, area, bot, top, bot, top, right, left, br, tr, bl)


def solution(mesh):
    counts = (mesh.shape["py"], mesh.shape["px"])
    p4, p3 = P(None, None, "py", "px"), P(None, "py", "px")
    return jax.shard_map(
        lambda *args: local(counts, *args),
        mesh=mesh,
        in_specs=(p4, p3, p4, p3, p3, p3, P("py", "px"), p4, p3),
        out_specs=(p4, p3, p3, p4),
        check_vma=False,
    )
```
